32 devices in a mesh: pa: 16 (over z, y, core), pb: 2 (over x).
Axes of the slice: x: 2, y: 2, z: 4, core: 2. Of those that a mesh axis runs over, the one named last changes fastest.
Arguments:
- sources: float32 [4096, 128], P(('pa', 'pb')), may hold values from -3 to 3, as said below
- targets: bfloat16 [4096, 128], P(('pa', 'pb')), may hold values from -2 to 2, as said below
- source_mass: float32 [4096], P(('pa', 'pb')), may hold values from -1 to 1
- target_mass: float32 [4096], P(('pa', 'pb')), may hold values from -1 to 1
Outputs:
- moved: float32 [4096, 128], P(('pa', 'pb'))
- dual_source: float32 [4096], P(('pa', 'pb'))
- dual_target: float32 [4096], P(('pa', 'pb'))
The draws below stay inside these ranges and needn't reach their ends.
Inputs may be any that keep to these rules, and one draw needn't show every extreme that they name: `targets`: each block of 128 target rows is drawn around one cluster centre, a different one for each block. `sources`: each block of 128 source rows is drawn around a cluster centre of its own, drawn independently of the target centres, possibly offset by a common shift.
All inputs are finite; a program needn't handle non-finite values.
Results may differ from the reference program's by a relative error of at most 0.003.
Values may be sent and summed in bfloat16 or wider, within the bound.
A program may use at most 64 MiB of HBM per device.

```python
import math
import jax
import jax.numpy as jnp
from jax import lax

D = 128
PTS_DEV = 128
STEPS = 1
ITERS = 2
POINTS = 4096
CLUSTERS = 32


def centre_spread():
    return 0.6 ** 0.5 / D ** 0.25


def cluster_centres(key, salt):
    return centre_spread() * jax.random.truncated_normal(jax.random.fold_in(key, salt), -3.5, 3.5, (CLUSTERS, D), jnp.float32)


def draw_targets(key, part):
    centres = cluster_centres(key, 101)
    owners = jnp.arange(POINTS, dtype=jnp.int32) // PTS_DEV
    noise = 0.1 * jax.random.truncated_normal(jax.random.fold_in(key, 202), -4.0, 4.0, (POINTS, D), jnp.float32)
    return (centres[owners] + noise).astype(jnp.bfloat16)


def draw_sources(key, part):
    centres = cluster_centres(key, 303)
    owners = jnp.arange(POINTS, dtype=jnp.int32) // PTS_DEV
    noise = 0.1 * jax.random.truncated_normal(jax.random.fold_in(key, 404), -4.0, 4.0, (POINTS, D), jnp.float32)
    points = centres[owners] + noise
    return points.astype(jnp.float32)


def steps_of(key, dims, pieces, least, largest):
    level, own = 1.0, jax.random.fold_in(key, 6)
    for position, blocks in pieces:
        draws = jnp.exp(jax.random.uniform(jax.random.fold_in(own, position), (blocks,), jnp.float32, least / len(pieces), largest / len(pieces)))
        level = level * jnp.repeat(draws, dims[position] // blocks).reshape([-1 if axis == position else 1 for axis in range(len(dims))])
    return level


def setup_inputs(seed: int = 0) -> dict:
    keys = jax.random.split(jax.random.key(seed), 5)
    sources = draw_sources(jax.random.fold_in(keys[4], 71), 0)
    targets = draw_targets(jax.random.fold_in(keys[4], 71), 0)
    source_mass = jnp.clip(jax.random.uniform(keys[2], (POINTS,), jnp.float32, -1.0, 1.0) * steps_of(keys[2], (POINTS,), ((0, 32),), -0.4, 0.0), -1.0, 1.0)
    target_mass = jnp.clip(jax.random.uniform(keys[3], (POINTS,), jnp.float32, -1.0, 1.0) * steps_of(keys[3], (POINTS,), ((0, 32),), -0.4, 0.0), -1.0, 1.0)
    return {"sources": sources, "targets": targets, "source_mass": source_mass, "target_mass": target_mass}


step_rate = 0.25


def squares(coords):
    wide = coords.astype(jnp.float32)
    return jnp.sum(wide * wide, axis=1)


def pair_cost(left, left_norm, right, right_norm):
    inner = lax.dot_general(left, right, (((1,), (1,)), ((), ())), preferred_element_type=jnp.float32)
    return left_norm[:, None] + right_norm[None, :] - 2.0 * inner


def row_lse(rows, row_norm, columns, column_norm, column_pot, block_rows):
    block_count = rows.shape[0] // block_rows

    def single(packed):
        block, block_norm = packed
        scores = column_pot[None, :] - pair_cost(block, block_norm, columns, column_norm)
        highest = jnp.max(scores, axis=1)
        return highest + jnp.log(jnp.sum(jnp.exp(scores - highest[:, None]), axis=1))

    packed = (rows.reshape(block_count, block_rows, rows.shape[1]), row_norm.reshape(block_count, block_rows))
    return lax.map(single, packed).reshape(rows.shape[0])


def plan_centres(rows, row_norm, row_pot, columns, column_norm, column_pot, block_rows):
    block_count = rows.shape[0] // block_rows

    def single(packed):
        block, block_norm, block_pot = packed
        cost = pair_cost(block, block_norm, columns, column_norm)
        weights = jnp.exp(block_pot[:, None] + column_pot[None, :] - cost).astype(jnp.bfloat16)
        return jnp.dot(weights, columns, preferred_element_type=jnp.float32)

    packed = (rows.reshape(block_count, block_rows, rows.shape[1]), row_norm.reshape(block_count, block_rows), row_pot.reshape(block_count, block_rows))
    return lax.map(single, packed).reshape(rows.shape[0], columns.shape[1])


def reference(sources, targets, source_mass, target_mass):
    block_rows = math.gcd(POINTS, 512)
    target_norm = squares(targets)
    moving = sources
    dual_target = jnp.zeros((POINTS,), jnp.float32)
    dual_source = jnp.zeros((POINTS,), jnp.float32)
    for flow_step in range(STEPS):
        coarse = moving.astype(jnp.bfloat16)
        coarse_norm = squares(coarse)
        shifted = dual_target + target_mass
        for sweep in range(ITERS + 1):
            shifted = dual_target + target_mass
            dual_source = -row_lse(coarse, coarse_norm, targets, target_norm, shifted, block_rows)
            if sweep < ITERS:
                lifted = dual_source + source_mass
                dual_target = -row_lse(targets, target_norm, coarse, coarse_norm, lifted, block_rows)
        centre = plan_centres(coarse, coarse_norm, dual_source, targets, target_norm, shifted, block_rows)
        moving = moving - 2.0 * step_rate * (moving - centre)
    return moving, dual_source, dual_target
```

```python
import functools

import jax
import jax.numpy as jnp
from jax import lax
from jax.experimental import pallas as pl
from jax.experimental.pallas import tpu as pltpu
from jax.sharding import PartitionSpec as P

MESH = pl.DeviceIdType.MESH
STEP_RATE = 0.25
LOG2E = 1.4426950408889634
LN2 = 0.6931471805599453


def lse2(parts):
    high = functools.reduce(jnp.maximum, parts)
    total = functools.reduce(jnp.add, [jnp.exp2(part - high) for part in parts])
    return high + jnp.log2(total)


def spread(row, size):
    return jnp.broadcast_to(row, (size, row.shape[1])).T


def kernel(
    cores, n_pb, n_r,
    src_ref, tgt_ref, smass_ref, tmass_ref,
    moved_ref, ds_ref, dt_ref,
    rows_buf, tgt_buf, small_s, small_r, gram, acol, lane_m, lane_s, weights,
    v_own, v_in, u_own, u_in, u_sum, p_out, p_in,
    rs_send, rs_recv, ss_send, ss_recv, tg_send, tg_recv, fw_send, fw_recv,
    rb_send, rb_recv, v_send, v_recv, u_send, u_recv, p_send, p_recv,
):
    n_s = cores * n_pb
    pts = src_ref.shape[0]
    pa = lax.axis_index("pa")
    pb = lax.axis_index("pb")
    r = pa // cores
    core = lax.rem(pa, cores)
    s = core * n_pb + pb
    half = n_r // 2
    hi = r // 2
    lo = lax.rem(r, 2)

    def row_peer(k):
        other = lax.rem(s + k, n_s)
        return {"pa": r * cores + other // n_pb, "pb": lax.rem(other, n_pb)}

    def col_index(k):
        return lax.rem(r + k, n_r)

    def col_peer(k):
        return {"pa": col_index(k) * cores + core, "pb": pb}

    def by_r(index):
        return {"pa": index * cores + core, "pb": pb}

    def copy(src, dst, send, recv, where):
        return pltpu.make_async_remote_copy(
            src_ref=src, dst_ref=dst, send_sem=send, recv_sem=recv,
            device_id=where, device_id_type=MESH,
        )

    barrier = pltpu.get_barrier_semaphore()
    for k in range(1, n_r):
        pl.semaphore_signal(barrier, inc=1, device_id=col_peer(k), device_id_type=MESH)
    for k in range(1, n_s):
        pl.semaphore_signal(barrier, inc=1, device_id=row_peer(k), device_id_type=MESH)

    rows_buf[s] = src_ref[...].astype(jnp.bfloat16)
    tgt_buf[r] = tgt_ref[...]
    wide = tgt_ref[...].astype(jnp.float32)
    tnorm = jnp.sum((wide * wide).T, axis=0, keepdims=True)
    mass = tmass_ref[...]
    small_r[r] = jnp.concatenate(
        [mass * LOG2E, (mass - tnorm) * LOG2E, jnp.zeros((6, pts), jnp.float32)], axis=0
    )
    small_s[s] = jnp.broadcast_to(smass_ref[...] * LOG2E, (8, pts))

    pl.semaphore_wait(barrier, n_r - 1 + n_s - 1)

    sends = []

    def start(*args):
        item = copy(*args)
        item.start()
        sends.append(item)
        return item

    partner = r + 1 - 2 * lo
    tg = {}
    for h in range(half - 1, 0, -1):
        where = lax.rem(hi + h, half) * 2 + lo
        tg[h] = start(tgt_buf.at[r], tgt_buf.at[r], tg_send.at[h], tg_recv.at[h], by_r(where))
    row_copies = [
        start(rows_buf.at[s], rows_buf.at[s], rs_send.at[k], rs_recv.at[k], row_peer(k))
        for k in range(1, n_s)
    ]
    fw = {0: start(tgt_buf.at[r], tgt_buf.at[r], fw_send.at[0], fw_recv.at[0], by_r(partner))}
    small_r_copies = [
        start(small_r.at[r], small_r.at[r], rb_send.at[k], rb_recv.at[k], col_peer(k))
        for k in range(1, n_r)
    ]
    small_s_copies = [
        start(small_s.at[s], small_s.at[s], ss_send.at[k], ss_recv.at[k], row_peer(k))
        for k in range(1, n_s)
    ]

    def gram_block(index):
        rows = rows_buf[...].reshape(n_s * pts, rows_buf.shape[2])
        inner = lax.dot_general(
            rows, tgt_buf[index], (((1,), (1,)), ((), ())), preferred_element_type=jnp.float32
        )
        gram[index] = inner * (2.0 * LOG2E)

    for item in row_copies:
        item.wait_recv()
    gram_block(r)
    fw[0].wait_recv()
    gram_block(partner)
    for h in range(1, half):
        tg[h].wait_recv()
        origin = lax.rem(hi - h + half, half) * 2
        fw[h] = start(
            tgt_buf.at[origin + lo], tgt_buf.at[origin + lo],
            fw_send.at[h], fw_recv.at[h], by_r(partner),
        )
        gram_block(origin + lo)
    for h in range(1, half):
        fw[h].wait_recv()
        gram_block(lax.rem(hi - h + half, half) * 2 + 1 - lo)
    for item in small_r_copies:
        item.wait_recv()
    for item in small_s_copies:
        item.wait_recv()

    chunk = 64 if n_r <= 8 else 8

    def row_partial(bvec, where):
        def step(i, carry):
            at = pl.ds(pl.multiple_of(i * chunk, chunk), chunk)
            parts = [gram[b, at, :] + bvec[b] for b in range(n_r)]
            high = functools.reduce(jnp.maximum, parts)
            lane_m[at, :] = high
            lane_s[at, :] = functools.reduce(jnp.add, [jnp.exp2(p - high) for p in parts])
            return carry

        lax.fori_loop(0, n_s * pts // chunk, step, 0)
        outs = []
        for q in range(n_s):
            at = slice(q * pts, (q + 1) * pts)
            high = lane_m[at, :].T
            top = jnp.max(high, axis=0, keepdims=True)
            total = jnp.sum(lane_s[at, :].T * jnp.exp2(high - top), axis=0, keepdims=True)
            outs.append(top + jnp.log2(total))
        pad = [jnp.zeros((1, pts), jnp.float32)] * (-n_s % 8)
        v_own[where] = jnp.concatenate(outs + pad, axis=0)
        return [
            start(
                v_own.at[where], v_in.at[where, k],
                v_send.at[where, k], v_recv.at[where, k], row_peer(k),
            )
            for k in range(1, n_s)
        ]

    def row_total(copies, where):
        for item in copies:
            item.wait_recv()
        return lse2([v_own[where]] + [v_in[where, k] for k in range(1, n_s)])

    def col_update(where):
        def one(b):
            x = (gram[b] + acol[...]).reshape(n_s * pts // 8, 8, pts)
            high = jnp.max(x, axis=0)
            total = jnp.sum(jnp.exp2(x - high[None]), axis=0)
            top = jnp.max(high, axis=0, keepdims=True)
            total = jnp.sum(total * jnp.exp2(high - top), axis=0, keepdims=True)
            u_own[where, pl.ds(b, 1), :] = top + jnp.log2(total)

        def step(b, carry):
            one(b)
            return carry

        lax.fori_loop(0, n_r, step, 0)
        copies = [
            start(
                u_own.at[where], u_in.at[where, k],
                u_send.at[where, k], u_recv.at[where, k], col_peer(k),
            )
            for k in range(1, n_r)
        ]
        for item in copies:
            item.wait_recv()
        return lse2([u_own[where]] + [u_in[where, k] for k in range(1, n_r)])

    iters = u_own.shape[0]
    bvec = [small_r[b, 1:2, :] for b in range(n_r)]
    for sweep in range(iters):
        v = row_total(row_partial(bvec, sweep), sweep)
        for q in range(n_s):
            acol[q * pts : (q + 1) * pts, :] = spread(small_s[q, 0:1, :] - v[q : q + 1, :], pts)
        u = col_update(sweep)
        u_sum[...] = u
        bvec = [small_r[b, 0:1, :] - u[b : b + 1, :] for b in range(n_r)]

    v_copies = row_partial(bvec, iters)
    for q in range(n_s):
        acol[q * pts : (q + 1) * pts, :] = spread(v_own[iters, q : q + 1, :], pts)

    p_copies = {}
    own_part = None
    for k in list(range(1, n_s)) + [0]:
        q = lax.rem(s + k, n_s)
        at = pl.ds(pl.multiple_of(q * pts, pts), pts)
        base = acol[at, :]
        for b in range(n_r):
            weights[:, b * pts : (b + 1) * pts] = jnp.exp2(
                gram[b, at, :] + bvec[b] - base
            ).astype(jnp.bfloat16)
        part = jnp.dot(
            weights[...],
            tgt_buf[...].reshape(n_r * pts, tgt_buf.shape[2]),
            preferred_element_type=jnp.float32,
        )
        if k:
            p_out[k] = part.astype(jnp.bfloat16)
            p_copies[k] = start(p_out.at[k], p_in.at[k], p_send.at[k], p_recv.at[k], row_peer(k))
        else:
            own_part = part

    own_src = rows_buf[s].astype(jnp.float32)
    snorm = jnp.sum((own_src * own_src).T, axis=0, keepdims=True)
    dt_ref[...] = tnorm - LN2 * u_sum[pl.ds(r, 1), :]
    for item in v_copies:
        item.wait_recv()
    mine = [v_own[iters, pl.ds(s, 1), :]] + [
        v_in[iters, k, pl.ds(s, 1), :] for k in range(1, n_s)
    ]
    total = lse2(mine)
    ds_ref[...] = snorm - LN2 * total
    centre = spread(jnp.exp2(mine[0] - total), pts) * own_part
    for k in range(1, n_s):
        scale = spread(jnp.exp2(mine[k] - total), pts)
        p_copies[k].wait_recv()
        centre = centre + scale * p_in[k].astype(jnp.float32)
    moving = src_ref[...]
    moved_ref[...] = moving - 2.0 * STEP_RATE * (moving - centre)
    for item in sends:
        item.wait_send()


ITERS = 2


def solution(mesh):
    n_pa, n_pb = mesh.shape["pa"], mesh.shape["pb"]
    cores = 2
    n_r = n_pa // cores
    n_s = cores * n_pb

    def body(sources, targets, source_mass, target_mass):
        pts, dim = sources.shape
        rows8 = -(-n_s // 8) * 8
        dma = pltpu.SemaphoreType.DMA
        f32, bf16 = jnp.float32, jnp.bfloat16
        vmem = pl.BlockSpec(memory_space=pltpu.VMEM)
        moved, ds, dt = pl.pallas_call(
            functools.partial(kernel, cores, n_pb, n_r),
            out_shape=(
                jax.ShapeDtypeStruct((pts, dim), f32),
                jax.ShapeDtypeStruct((1, pts), f32),
                jax.ShapeDtypeStruct((1, pts), f32),
            ),
            in_specs=[vmem] * 4,
            out_specs=(vmem,) * 3,
            scratch_shapes=[
                pltpu.VMEM((n_s, pts, dim), bf16),
                pltpu.VMEM((n_r, pts, dim), bf16),
                pltpu.VMEM((n_s, 8, pts), f32),
                pltpu.VMEM((n_r, 8, pts), f32),
                pltpu.VMEM((n_r, n_s * pts, pts), f32),
                pltpu.VMEM((n_s * pts, pts), f32),
                pltpu.VMEM((n_s * pts, pts), f32),
                pltpu.VMEM((n_s * pts, pts), f32),
                pltpu.VMEM((pts, n_r * pts), bf16),
                pltpu.VMEM((ITERS + 1, rows8, pts), f32),
                pltpu.VMEM((ITERS + 1, n_s, rows8, pts), f32),
                pltpu.VMEM((ITERS, n_r, pts), f32),
                pltpu.VMEM((ITERS, n_r, n_r, pts), f32),
                pltpu.VMEM((n_r, pts), f32),
                pltpu.VMEM((n_s, pts, dim), bf16),
                pltpu.VMEM((n_s, pts, dim), bf16),
                dma((n_s,)), dma((n_s,)), dma((n_s,)), dma((n_s,)),
                dma((n_r,)), dma((n_r,)), dma((n_r,)), dma((n_r,)),
                dma((n_r,)), dma((n_r,)),
                dma((ITERS + 1, n_s)), dma((ITERS + 1, n_s)),
                dma((ITERS, n_r)), dma((ITERS, n_r)),
                dma((n_s,)), dma((n_s,)),
            ],
            compiler_params=pltpu.CompilerParams(
                collective_id=0, has_side_effects=True, vmem_limit_bytes=60 * 1024 * 1024
            ),
        )(sources, targets, source_mass[None, :], target_mass[None, :])
        return moved, ds[0], dt[0]

    return jax.shard_map(
        body,
        mesh=mesh,
        in_specs=(P(("pa", "pb"), None), P(("pa", "pb"), None), P(("pa", "pb")), P(("pa", "pb"))),
        out_specs=(P(("pa", "pb"), None), P(("pa", "pb")), P(("pa", "pb"))),
        check_vma=False,
    )
```

```python
import functools

import jax
import jax.numpy as jnp
from jax import lax
from jax.experimental import pallas as pl
from jax.experimental.pallas import tpu as pltpu
from jax.sharding import PartitionSpec as P

MESH = pl.DeviceIdType.MESH
STEP_RATE = 0.25
LOG2E = 1.4426950408889634
LN2 = 0.6931471805599453
EXTRA = 16


def lse2(parts):
    high = functools.reduce(jnp.maximum, parts)
    total = functools.reduce(jnp.add, [jnp.exp2(part - high) for part in parts])
    return high + jnp.log2(total)


def spread(row, size):
    return jnp.broadcast_to(row, (size, row.shape[1])).T


def pack_rows(rows):
    pieces = []
    for row in rows:
        for _ in range(3):
            part = row.astype(jnp.bfloat16).astype(jnp.float32)
            pieces.append(part)
            row = row - part
    pad = jnp.zeros((EXTRA - len(pieces), rows[0].shape[1]), jnp.float32)
    return jnp.concatenate(pieces + [pad], axis=0).astype(jnp.bfloat16)


def unpack_row(buf, index, start, which):
    rows = buf[index, start:, :].astype(jnp.float32)
    at = 3 * which
    return rows[at : at + 1] + rows[at + 1 : at + 2] + rows[at + 2 : at + 3]


def finish(moved_in, ds_in, dt_in, moved_ref, ds_ref, dt_ref):
    moved_ref[...] = moved_in[...]
    ds_ref[...] = ds_in[...]
    dt_ref[...] = dt_in[...]


def repeat(count, unrolled, step):
    if unrolled:
        for i in range(count):
            step(i, 0)
    else:
        lax.fori_loop(0, count, step, 0)


def kernel(
    cores, n_pb, n_r,
    src_hbm, tgt_hbm, smass_hbm, tmass_hbm,
    moved_ref, ds_ref, dt_ref,
    src_ref, tgt_ref, smass_ref, tmass_ref, load_sem,
    rows_pk, tgt_pk, rows_buf, tgt_buf, gram, acol, lane_m, lane_s, weights,
    v_own, v_in, u_own, u_in, u_sum, p_out, p_in,
    rs_send, rs_recv, tg_send, tg_recv, fw_send, fw_recv, v_send, v_recv, u_send, u_recv, p_send, p_recv,
):
    n_s = cores * n_pb
    pts = src_ref.shape[0]
    loads = [
        pltpu.make_async_copy(a, b, load_sem.at[i])
        for i, (a, b) in enumerate(
            [(tgt_hbm, tgt_ref), (tmass_hbm, tmass_ref), (src_hbm, src_ref), (smass_hbm, smass_ref)]
        )
    ]
    pa = lax.axis_index("pa")
    pb = lax.axis_index("pb")
    r = pa // cores
    core = lax.rem(pa, cores)
    s = core * n_pb + pb
    half = n_r // 2
    hi = r // 2
    lo = lax.rem(r, 2)

    def row_peer(k):
        other = lax.rem(s + k, n_s)
        return {"pa": r * cores + other // n_pb, "pb": lax.rem(other, n_pb)}

    def col_index(k):
        return lax.rem(r + k, n_r)

    def col_peer(k):
        return {"pa": col_index(k) * cores + core, "pb": pb}

    def by_r(index):
        return {"pa": index * cores + core, "pb": pb}

    def copy(src, dst, send, recv, where):
        return pltpu.make_async_remote_copy(
            src_ref=src, dst_ref=dst, send_sem=send, recv_sem=recv,
            device_id=where, device_id_type=MESH,
        )

    partner = r + 1 - 2 * lo

    def line(h):
        return lax.rem(hi + h, half) * 2 + lo

    barrier = pltpu.get_barrier_semaphore()
    peers = [by_r(line(h)) for h in range(1, half)] + [by_r(partner)]
    peers += [row_peer(k) for k in range(1, n_s)]
    for where in peers:
        pl.semaphore_signal(barrier, inc=1, device_id=where, device_id_type=MESH)
    for item in loads:
        item.start()
    for item in loads:
        item.wait()

    tgt_pk[r, :pts, :] = tgt_ref[...]
    wide = tgt_ref[...].astype(jnp.float32)
    tnorm = jnp.sum((wide * wide).T, axis=0, keepdims=True)
    mass = tmass_ref[...]
    tgt_pk[r, pts:, :] = pack_rows([mass * LOG2E, (mass - tnorm) * LOG2E])
    rows_pk[s, :pts, :] = src_ref[...].astype(jnp.bfloat16)
    rows_pk[s, pts:, :] = pack_rows([smass_ref[...] * LOG2E])

    pl.semaphore_wait(barrier, len(peers))

    sends = []

    def start(*args):
        item = copy(*args)
        item.start()
        sends.append(item)
        return item

    along = {
        h: start(
            tgt_pk.at[r], tgt_pk.at[r], tg_send.at[h], tg_recv.at[h], by_r(line(h))
        )
        for h in range(1, half)
    }
    across = {
        0: start(tgt_pk.at[r], tgt_pk.at[r], fw_send.at[0], fw_recv.at[0], by_r(partner))
    }
    row_copies = [
        start(rows_pk.at[s], rows_pk.at[s], rs_send.at[k], rs_recv.at[k], row_peer(k))
        for k in range(1, n_s)
    ]

    def gram_block(index):
        inner = lax.dot_general(
            rows_buf[...], tgt_pk[index, :pts, :], (((1,), (1,)), ((), ())),
            preferred_element_type=jnp.float32,
        )
        gram[index] = inner * (2.0 * LOG2E)
        tgt_buf[index] = tgt_pk[index, :pts, :]

    for item in row_copies:
        item.wait_recv()
    for q in range(n_s):
        rows_buf[q * pts : (q + 1) * pts, :] = rows_pk[q, :pts, :]
    gram_block(r)
    for h in range(1, half):
        along[h].wait_recv()
        block = line(half - h)
        across[h] = start(
            tgt_pk.at[block], tgt_pk.at[block], fw_send.at[h], fw_recv.at[h], by_r(partner)
        )
        gram_block(block)
    for h in range(half):
        across[h].wait_recv()
        gram_block(line(half - h) + 1 - 2 * lo)

    chunk = 16

    def row_partial(bvec, where):
        def step(i, carry):
            first = i * chunk if isinstance(i, int) else pl.multiple_of(i * chunk, chunk)
            at = pl.ds(first, chunk)
            parts = [gram[b, at, :] + bvec[b] for b in range(n_r)]
            high = functools.reduce(jnp.maximum, parts)
            lane_m[at, :] = high
            lane_s[at, :] = functools.reduce(jnp.add, [jnp.exp2(p - high) for p in parts])
            return carry

        repeat(n_s * pts // chunk, n_r <= 8, step)
        outs = []
        for q in range(n_s):
            at = slice(q * pts, (q + 1) * pts)
            high = lane_m[at, :].T
            top = jnp.max(high, axis=0, keepdims=True)
            total = jnp.sum(lane_s[at, :].T * jnp.exp2(high - top), axis=0, keepdims=True)
            outs.append(top + jnp.log2(total))
        pad = [jnp.zeros((1, pts), jnp.float32)] * (-n_s % 8)
        v_own[where] = jnp.concatenate(outs + pad, axis=0)
        return [
            start(
                v_own.at[where], v_in.at[where, k],
                v_send.at[where, k], v_recv.at[where, k], row_peer(k),
            )
            for k in range(1, n_s)
        ]

    def row_total(copies, where):
        for item in copies:
            item.wait_recv()
        return lse2([v_own[where]] + [v_in[where, k] for k in range(1, n_s)])

    def col_update(where):
        def one(b):
            x = (gram[b] + acol[...]).reshape(n_s * pts // 8, 8, pts)
            high = jnp.max(x, axis=0)
            total = jnp.sum(jnp.exp2(x - high[None]), axis=0)
            top = jnp.max(high, axis=0, keepdims=True)
            total = jnp.sum(total * jnp.exp2(high - top), axis=0, keepdims=True)
            u_own[where, pl.ds(b, 1), :] = top + jnp.log2(total)

        def step(b, carry):
            one(b)
            return carry

        repeat(n_r, n_r <= 8, step)
        copies = [
            start(
                u_own.at[where], u_in.at[where, k],
                u_send.at[where, k], u_recv.at[where, k], col_peer(k),
            )
            for k in range(1, n_r)
        ]
        for item in copies:
            item.wait_recv()
        return lse2([u_own[where]] + [u_in[where, k] for k in range(1, n_r)])

    iters = u_own.shape[0]
    bvec = [unpack_row(tgt_pk, b, pts, 1) for b in range(n_r)]
    for sweep in range(iters):
        v = row_total(row_partial(bvec, sweep), sweep)
        for q in range(n_s):
            acol[q * pts : (q + 1) * pts, :] = spread(unpack_row(rows_pk, q, pts, 0) - v[q : q + 1, :], pts)
        u = col_update(sweep)
        u_sum[...] = u
        bvec = [unpack_row(tgt_pk, b, pts, 0) - u[b : b + 1, :] for b in range(n_r)]

    v_copies = row_partial(bvec, iters)
    for q in range(n_s):
        acol[q * pts : (q + 1) * pts, :] = spread(v_own[iters, q : q + 1, :], pts)

    p_copies = {}
    own_part = None
    for k in list(range(1, n_s)) + [0]:
        q = lax.rem(s + k, n_s)
        at = pl.ds(pl.multiple_of(q * pts, pts), pts)
        base = acol[at, :]
        for b in range(n_r):
            weights[:, b * pts : (b + 1) * pts] = jnp.exp2(
                gram[b, at, :] + bvec[b] - base
            ).astype(jnp.bfloat16)
        part = jnp.dot(
            weights[...],
            tgt_buf[...].reshape(n_r * pts, tgt_buf.shape[2]),
            preferred_element_type=jnp.float32,
        )
        if k:
            p_out[k] = part.astype(jnp.bfloat16)
            p_copies[k] = start(p_out.at[k], p_in.at[k], p_send.at[k], p_recv.at[k], row_peer(k))
        else:
            own_part = part

    own_src = rows_pk[s, :pts, :].astype(jnp.float32)
    snorm = jnp.sum((own_src * own_src).T, axis=0, keepdims=True)
    dt_ref[...] = tnorm - LN2 * u_sum[pl.ds(r, 1), :]
    for item in v_copies:
        item.wait_recv()
    mine = [v_own[iters, pl.ds(s, 1), :]] + [
        v_in[iters, k, pl.ds(s, 1), :] for k in range(1, n_s)
    ]
    total = lse2(mine)
    ds_ref[...] = snorm - LN2 * total
    centre = spread(jnp.exp2(mine[0] - total), pts) * own_part
    for k in range(1, n_s):
        scale = spread(jnp.exp2(mine[k] - total), pts)
        p_copies[k].wait_recv()
        centre = centre + scale * p_in[k].astype(jnp.float32)
    moving = src_ref[...]
    moved_ref[...] = moving - 2.0 * STEP_RATE * (moving - centre)
    for item in sends:
        item.wait_send()


ITERS = 2


def solution(mesh):
    n_pa, n_pb = mesh.shape["pa"], mesh.shape["pb"]
    cores = 2
    n_r = n_pa // cores
    n_s = cores * n_pb

    def body(sources, targets, source_mass, target_mass):
        pts, dim = sources.shape
        rows8 = -(-n_s // 8) * 8
        dma = pltpu.SemaphoreType.DMA
        f32, bf16 = jnp.float32, jnp.bfloat16
        vmem = pl.BlockSpec(memory_space=pltpu.VMEM)
        results = (
            jax.ShapeDtypeStruct((pts, dim), f32),
            jax.ShapeDtypeStruct((1, pts), f32),
            jax.ShapeDtypeStruct((1, pts), f32),
        )
        parts = pl.pallas_call(
            functools.partial(kernel, cores, n_pb, n_r),
            out_shape=results,
            in_specs=[pl.BlockSpec(memory_space=pl.ANY)] * 4,
            out_specs=(vmem,) * 3,
            scratch_shapes=[
                pltpu.VMEM((pts, dim), f32),
                pltpu.VMEM((pts, dim), bf16),
                pltpu.VMEM((1, pts), f32),
                pltpu.VMEM((1, pts), f32),
                dma((4,)),
                pltpu.VMEM((n_s, pts + EXTRA, dim), bf16),
                pltpu.VMEM((n_r, pts + EXTRA, dim), bf16),
                pltpu.VMEM((n_s * pts, dim), bf16),
                pltpu.VMEM((n_r, pts, dim), bf16),
                pltpu.VMEM((n_r, n_s * pts, pts), f32),
                pltpu.VMEM((n_s * pts, pts), f32),
                pltpu.VMEM((n_s * pts, pts), f32),
                pltpu.VMEM((n_s * pts, pts), f32),
                pltpu.VMEM((pts, n_r * pts), bf16),
                pltpu.VMEM((ITERS + 1, rows8, pts), f32),
                pltpu.VMEM((ITERS + 1, n_s, rows8, pts), f32),
                pltpu.VMEM((ITERS, n_r, pts), f32),
                pltpu.VMEM((ITERS, n_r, n_r, pts), f32),
                pltpu.VMEM((n_r, pts), f32),
                pltpu.VMEM((n_s, pts, dim), bf16),
                pltpu.VMEM((n_s, pts, dim), bf16),
                dma((n_s,)), dma((n_s,)),
                dma((n_r,)), dma((n_r,)), dma((n_r,)), dma((n_r,)),
                dma((ITERS + 1, n_s)), dma((ITERS + 1, n_s)),
                dma((ITERS, n_r)), dma((ITERS, n_r)),
                dma((n_s,)), dma((n_s,)),
            ],
            compiler_params=pltpu.CompilerParams(
                collective_id=0, has_side_effects=True, vmem_limit_bytes=60 * 1024 * 1024
            ),
        )(sources, targets, source_mass[None, :], target_mass[None, :])
        moved, ds, dt = pl.pallas_call(
            finish, out_shape=results, in_specs=[vmem] * 3, out_specs=(vmem,) * 3
        )(*parts)
        return moved, ds[0], dt[0]

    return jax.shard_map(
        body,
        mesh=mesh,
        in_specs=(P(("pa", "pb"), None), P(("pa", "pb"), None), P(("pa", "pb")), P(("pa", "pb"))),
        out_specs=(P(("pa", "pb"), None), P(("pa", "pb")), P(("pa", "pb"))),
        check_vma=False,
    )
```

```python
import functools

import jax
import jax.numpy as jnp
from jax import lax
from jax.experimental import pallas as pl
from jax.experimental.pallas import tpu as pltpu
from jax.sharding import PartitionSpec as P

MESH = pl.DeviceIdType.MESH
STEP_RATE = 0.25
LOG2E = 1.4426950408889634
LN2 = 0.6931471805599453
EXTRA = 16


def lse2(parts):
    high = functools.reduce(jnp.maximum, parts)
    total = functools.reduce(jnp.add, [jnp.exp2(part - high) for part in parts])
    return high + jnp.log2(total)


def spread(row, size):
    return jnp.broadcast_to(row, (size, row.shape[1])).T


def pack_rows(rows):
    pieces = []
    for row in rows:
        for _ in range(3):
            part = row.astype(jnp.bfloat16).astype(jnp.float32)
            pieces.append(part)
            row = row - part
    pad = jnp.zeros((EXTRA - len(pieces), rows[0].shape[1]), jnp.float32)
    return jnp.concatenate(pieces + [pad], axis=0).astype(jnp.bfloat16)


def unpack_row(buf, index, start, which):
    rows = buf[index, start:, :].astype(jnp.float32)
    at = 3 * which
    return rows[at : at + 1] + rows[at + 1 : at + 2] + rows[at + 2 : at + 3]


def finish(moved_in, ds_in, dt_in, moved_ref, ds_ref, dt_ref):
    moved_ref[...] = moved_in[...]
    ds_ref[...] = ds_in[...]
    dt_ref[...] = dt_in[...]


def repeat(count, unrolled, step):
    if unrolled:
        for i in range(count):
            step(i, 0)
    else:
        lax.fori_loop(0, count, step, 0)


def kernel(
    cores, n_pb, n_r,
    src_hbm, tgt_hbm, smass_hbm, tmass_hbm,
    moved_ref, ds_ref, dt_ref,
    src_ref, tgt_ref, smass_ref, tmass_ref, load_sem,
    rows_pk, tgt_pk, rows_buf, tgt_buf, gram, acol, lane_m, lane_s, weights,
    v_own, v_in, u_own, u_in, u_sum, p_out, p_in,
    rs_send, rs_recv, tg_send, tg_recv, fw_send, fw_recv, v_send, v_recv, u_send, u_recv, p_send, p_recv,
):
    n_s = cores * n_pb
    pts = src_ref.shape[0]
    loads = [
        pltpu.make_async_copy(a, b, load_sem.at[i])
        for i, (a, b) in enumerate(
            [(tgt_hbm, tgt_ref), (tmass_hbm, tmass_ref), (src_hbm, src_ref), (smass_hbm, smass_ref)]
        )
    ]
    pa = lax.axis_index("pa")
    pb = lax.axis_index("pb")
    r = pa // cores
    core = lax.rem(pa, cores)
    s = core * n_pb + pb
    half = n_r // 2
    hi = r // 2
    lo = lax.rem(r, 2)

    def row_peer(k):
        other = lax.rem(s + k, n_s)
        return {"pa": r * cores + other // n_pb, "pb": lax.rem(other, n_pb)}

    def col_index(k):
        return lax.rem(r + k, n_r)

    def col_peer(k):
        return {"pa": col_index(k) * cores + core, "pb": pb}

    def by_r(index):
        return {"pa": index * cores + core, "pb": pb}

    def copy(src, dst, send, recv, where):
        return pltpu.make_async_remote_copy(
            src_ref=src, dst_ref=dst, send_sem=send, recv_sem=recv,
            device_id=where, device_id_type=MESH,
        )

    partner = r + 1 - 2 * lo

    near = jnp.minimum(hi, half - 1 - hi)
    outer = jnp.where(hi > half - 1 - hi, -1, 1)

    def line(j):
        both = (j + 1) // 2 * (1 if j % 2 else -1)
        return (hi + jnp.where(j <= 2 * near, both, outer * (j - near))) * 2 + lo

    barrier = pltpu.get_barrier_semaphore()
    peers = [by_r(line(j)) for j in range(1, half)] + [by_r(partner)]
    peers += [row_peer(k) for k in range(1, n_s)]
    for where in peers:
        pl.semaphore_signal(barrier, inc=1, device_id=where, device_id_type=MESH)
    for item in loads:
        item.start()
    for item in loads:
        item.wait()

    tgt_pk[r, :pts, :] = tgt_ref[...]
    wide = tgt_ref[...].astype(jnp.float32)
    tnorm = jnp.sum((wide * wide).T, axis=0, keepdims=True)
    mass = tmass_ref[...]
    tgt_pk[r, pts:, :] = pack_rows([mass * LOG2E, (mass - tnorm) * LOG2E])
    rows_pk[s, :pts, :] = src_ref[...].astype(jnp.bfloat16)
    rows_pk[s, pts:, :] = pack_rows([smass_ref[...] * LOG2E])

    pl.semaphore_wait(barrier, len(peers))

    sends = []

    def start(*args):
        item = copy(*args)
        item.start()
        sends.append(item)
        return item

    for j in range(half - 1, 0, -1):
        start(tgt_pk.at[r], tgt_pk.at[r], tg_send.at[j], tg_recv.at[r], by_r(line(j)))
    across = {
        0: start(tgt_pk.at[r], tgt_pk.at[r], fw_send.at[0], fw_recv.at[0], by_r(partner))
    }
    row_copies = [
        start(rows_pk.at[s], rows_pk.at[s], rs_send.at[k], rs_recv.at[k], row_peer(k))
        for k in range(1, n_s)
    ]

    def gram_block(index):
        inner = lax.dot_general(
            rows_buf[...], tgt_pk[index, :pts, :], (((1,), (1,)), ((), ())),
            preferred_element_type=jnp.float32,
        )
        gram[index] = inner * (2.0 * LOG2E)
        tgt_buf[index] = tgt_pk[index, :pts, :]

    for item in row_copies:
        item.wait_recv()
    for q in range(n_s):
        rows_buf[q * pts : (q + 1) * pts, :] = rows_pk[q, :pts, :]
    gram_block(r)
    for j in range(1, half):
        block = line(j)
        landed = tgt_pk.at[block]
        copy(landed, landed, tg_send.at[j], tg_recv.at[block], by_r(block)).wait_recv()
        across[j] = start(landed, landed, fw_send.at[j], fw_recv.at[j], by_r(partner))
        gram_block(block)
    for j in range(half):
        across[j].wait_recv()
        gram_block(line(j) + 1 - 2 * lo)

    chunk = 16

    def row_partial(bvec, where):
        def step(i, carry):
            first = i * chunk if isinstance(i, int) else pl.multiple_of(i * chunk, chunk)
            at = pl.ds(first, chunk)
            parts = [gram[b, at, :] + bvec[b] for b in range(n_r)]
            high = functools.reduce(jnp.maximum, parts)
            lane_m[at, :] = high
            lane_s[at, :] = functools.reduce(jnp.add, [jnp.exp2(p - high) for p in parts])
            return carry

        repeat(n_s * pts // chunk, n_r <= 8, step)
        outs = []
        for q in range(n_s):
            at = slice(q * pts, (q + 1) * pts)
            high = lane_m[at, :].T
            top = jnp.max(high, axis=0, keepdims=True)
            total = jnp.sum(lane_s[at, :].T * jnp.exp2(high - top), axis=0, keepdims=True)
            outs.append(top + jnp.log2(total))
        pad = [jnp.zeros((1, pts), jnp.float32)] * (-n_s % 8)
        v_own[where] = jnp.concatenate(outs + pad, axis=0)
        return [
            start(
                v_own.at[where], v_in.at[where, k],
                v_send.at[where, k], v_recv.at[where, k], row_peer(k),
            )
            for k in range(1, n_s)
        ]

    def row_total(copies, where):
        for item in copies:
            item.wait_recv()
        return lse2([v_own[where]] + [v_in[where, k] for k in range(1, n_s)])

    def col_update(where):
        def one(b):
            x = (gram[b] + acol[...]).reshape(n_s * pts // 8, 8, pts)
            high = jnp.max(x, axis=0)
            total = jnp.sum(jnp.exp2(x - high[None]), axis=0)
            top = jnp.max(high, axis=0, keepdims=True)
            total = jnp.sum(total * jnp.exp2(high - top), axis=0, keepdims=True)
            u_own[where, pl.ds(b, 1), :] = top + jnp.log2(total)

        def step(b, carry):
            one(b)
            return carry

        repeat(n_r, n_r <= 8, step)
        for at, index in enumerate(
            [line(j) + flip for j in range(half - 1, -1, -1) for flip in (1 - 2 * lo, 0)][:-1]
        ):
            start(
                u_own.at[where], u_in.at[where, r],
                u_send.at[where, at], u_recv.at[where, r], by_r(index),
            )
        others = [lax.rem(r + k, n_r) for k in range(1, n_r)]
        for index in others:
            landed = u_in.at[where, index]
            copy(
                u_own.at[where], landed, u_send.at[where, 0], u_recv.at[where, index], by_r(index)
            ).wait_recv()
        return lse2([u_own[where]] + [u_in[where, index] for index in others])

    iters = u_own.shape[0]
    bvec = [unpack_row(tgt_pk, b, pts, 1) for b in range(n_r)]
    for sweep in range(iters):
        v = row_total(row_partial(bvec, sweep), sweep)
        for q in range(n_s):
            acol[q * pts : (q + 1) * pts, :] = spread(unpack_row(rows_pk, q, pts, 0) - v[q : q + 1, :], pts)
        u = col_update(sweep)
        u_sum[...] = u
        bvec = [unpack_row(tgt_pk, b, pts, 0) - u[b : b + 1, :] for b in range(n_r)]

    v_copies = row_partial(bvec, iters)
    for q in range(n_s):
        acol[q * pts : (q + 1) * pts, :] = spread(v_own[iters, q : q + 1, :], pts)

    p_copies = {}
    own_part = None
    for k in sorted(range(1, n_s), key=lambda k: k % n_pb == 0) + [0]:
        q = lax.rem(s + k, n_s)
        at = pl.ds(pl.multiple_of(q * pts, pts), pts)
        base = acol[at, :]
        for b in range(n_r):
            weights[k, :, b * pts : (b + 1) * pts] = jnp.exp2(
                gram[b, at, :] + bvec[b] - base
            ).astype(jnp.bfloat16)
        part = jnp.dot(
            weights[k],
            tgt_buf[...].reshape(n_r * pts, tgt_buf.shape[2]),
            preferred_element_type=jnp.float32,
        )
        if k:
            p_out[k] = part.astype(jnp.bfloat16)
            p_copies[k] = start(p_out.at[k], p_in.at[k], p_send.at[k], p_recv.at[k], row_peer(k))
        else:
            own_part = part

    own_src = rows_pk[s, :pts, :].astype(jnp.float32)
    snorm = jnp.sum((own_src * own_src).T, axis=0, keepdims=True)
    dt_ref[...] = tnorm - LN2 * u_sum[pl.ds(r, 1), :]
    for item in v_copies:
        item.wait_recv()
    mine = [v_own[iters, pl.ds(s, 1), :]] + [
        v_in[iters, k, pl.ds(s, 1), :] for k in range(1, n_s)
    ]
    total = lse2(mine)
    ds_ref[...] = snorm - LN2 * total
    centre = spread(jnp.exp2(mine[0] - total), pts) * own_part
    for k in range(1, n_s):
        scale = spread(jnp.exp2(mine[k] - total), pts)
        p_copies[k].wait_recv()
        centre = centre + scale * p_in[k].astype(jnp.float32)
    moving = src_ref[...]
    moved_ref[...] = moving - 2.0 * STEP_RATE * (moving - centre)
    for item in sends:
        item.wait_send()


ITERS = 2


def solution(mesh):
    n_pa, n_pb = mesh.shape["pa"], mesh.shape["pb"]
    cores = 2
    n_r = n_pa // cores
    n_s = cores * n_pb

    def body(sources, targets, source_mass, target_mass):
        pts, dim = sources.shape
        rows8 = -(-n_s // 8) * 8
        dma = pltpu.SemaphoreType.DMA
        f32, bf16 = jnp.float32, jnp.bfloat16
        vmem = pl.BlockSpec(memory_space=pltpu.VMEM)
        results = (
            jax.ShapeDtypeStruct((pts, dim), f32),
            jax.ShapeDtypeStruct((1, pts), f32),
            jax.ShapeDtypeStruct((1, pts), f32),
        )
        parts = pl.pallas_call(
            functools.partial(kernel, cores, n_pb, n_r),
            out_shape=results,
            in_specs=[pl.BlockSpec(memory_space=pl.ANY)] * 4,
            out_specs=(vmem,) * 3,
            scratch_shapes=[
                pltpu.VMEM((pts, dim), f32),
                pltpu.VMEM((pts, dim), bf16),
                pltpu.VMEM((1, pts), f32),
                pltpu.VMEM((1, pts), f32),
                dma((4,)),
                pltpu.VMEM((n_s, pts + EXTRA, dim), bf16),
                pltpu.VMEM((n_r, pts + EXTRA, dim), bf16),
                pltpu.VMEM((n_s * pts, dim), bf16),
                pltpu.VMEM((n_r, pts, dim), bf16),
                pltpu.VMEM((n_r, n_s * pts, pts), f32),
                pltpu.VMEM((n_s * pts, pts), f32),
                pltpu.VMEM((n_s * pts, pts), f32),
                pltpu.VMEM((n_s * pts, pts), f32),
                pltpu.VMEM((n_s, pts, n_r * pts), bf16),
                pltpu.VMEM((ITERS + 1, rows8, pts), f32),
                pltpu.VMEM((ITERS + 1, n_s, rows8, pts), f32),
                pltpu.VMEM((ITERS, n_r, pts), f32),
                pltpu.VMEM((ITERS, n_r, n_r, pts), f32),
                pltpu.VMEM((n_r, pts), f32),
                pltpu.VMEM((n_s, pts, dim), bf16),
                pltpu.VMEM((n_s, pts, dim), bf16),
                dma((n_s,)), dma((n_s,)),
                dma((n_r,)), dma((n_r,)), dma((n_r,)), dma((n_r,)),
                dma((ITERS + 1, n_s)), dma((ITERS + 1, n_s)),
                dma((ITERS, n_r)), dma((ITERS, n_r)),
                dma((n_s,)), dma((n_s,)),
            ],
            compiler_params=pltpu.CompilerParams(
                collective_id=0, has_side_effects=True, vmem_limit_bytes=60 * 1024 * 1024
            ),
        )(sources, targets, source_mass[None, :], target_mass[None, :])
        moved, ds, dt = pl.pallas_call(
            finish, out_shape=results, in_specs=[vmem] * 3, out_specs=(vmem,) * 3
        )(*parts)
        return moved, ds[0], dt[0]

    return jax.shard_map(
        body,
        mesh=mesh,
        in_specs=(P(("pa", "pb"), None), P(("pa", "pb"), None), P(("pa", "pb")), P(("pa", "pb"))),
        out_specs=(P(("pa", "pb"), None), P(("pa", "pb")), P(("pa", "pb"))),
        check_vma=False,
    )
```
